32 devices in a mesh: row: 2 (over x), col: 16 (over z, y, core).
Axes of the slice: x: 2, y: 2, z: 4, core: 2. Of those that a mesh axis runs over, the one named last changes fastest.
Arguments:
- rhs_fields: float32 [4, 256, 4096], P(None, 'row', 'col'), may hold values from -6 to 6
- coupling: float32 [256, 4096], P('row', 'col'), may hold values from 1 to 8
- inv_pivot: float32 [2, 1024, 1024], P('row', 'col'), may hold values from -0.75 to 0.75
- lower_factor: float32 [2, 1024, 1024], P('row', 'col'), may hold values from -0.125 to 0.125
- upper_factor: float32 [2, 1024, 1024], P('row', 'col'), may hold values from -0.125 to 0.125
Outputs:
- correction: float32 [4, 256, 4096], P(None, 'row', 'col')
The draws below stay inside these ranges and needn't reach their ends.
All inputs are finite; a program needn't handle non-finite values.
Results may differ from the reference program's by a relative error of at most 0.0001.
Values sent between devices are 32-bit elements; how exact they have to be, the bound alone decides.
No kernel may reach another device: no remote copies, remote signals or barrier semaphores. Data moves between devices by JAX's collectives and lax.ppermute only.
A program may use at most 64 MiB of HBM per device.

```python
import math
import jax
import jax.numpy as jnp
from jax import lax

CX = 128
CY = 256
NRHS = 4
SWEEPS = 4
SUB = 8
NCB = 1024
NX = 256
NY = 4096
N_ROW = 2
N_COL = 16


def steps_of(key, shape, split, smallest, high):
    def one(dim, shards_of):
        draws = jax.random.uniform(jax.random.fold_in(jax.random.fold_in(key, 6), dim), (shards_of,), jnp.float32, smallest / len(split), high / len(split))
        return jnp.repeat(jnp.exp(draws), shape[dim] // shards_of).reshape((-1,) + (1,) * (len(shape) - dim - 1))

    level = one(*split[0])
    for cut in split[1:]:
        level = level * one(*cut)
    return level


def centred(stream_key, extent, spread, most, pieces=(), dtype=jnp.bfloat16):
    factor_of = steps_of(stream_key, extent, pieces, -0.22, 0.18) if pieces else 1.0
    entries = jax.random.normal(stream_key, extent, jnp.float32) * spread * factor_of
    return jnp.minimum(jnp.maximum(entries, -most), most).astype(dtype)


def setup_inputs(seed: int = 0) -> dict:
    key_of = jax.random.split(jax.random.key(seed), 6)
    return {
        "rhs_fields": centred(key_of[0], (NRHS, NX, NY), 1.0, 6.0, ((1, 2), (2, 16)), jnp.float32),
        "coupling": jnp.clip(jnp.exp(math.log(8.0) - 2.0794415 * jax.random.uniform(key_of[1], (NX, NY), jnp.float32) ** steps_of(key_of[1], (NX, NY), ((0, 2), (1, 16)), -0.2, 0.2)), 1.0, 8.0),
        "inv_pivot": centred(key_of[2], (N_ROW, NCB, NCB), (NCB // 16) ** -0.5, 0.75, ((0, 2), (1, 16)), jnp.float32),
        "lower_factor": centred(key_of[3], (N_ROW, NCB, NCB), (2 * NCB) ** -0.5, 0.125, ((0, 2), (1, 16)), jnp.float32),
        "upper_factor": centred(key_of[4], (N_ROW, NCB, NCB), (2 * NCB) ** -0.5, 0.125, ((0, 2), (1, 16)), jnp.float32),
    }


def face_terms(padded):
    center = padded[1:-1, 1:-1]
    upward = 0.5 * (center + padded[:-2, 1:-1])
    downward = 0.5 * (center + padded[2:, 1:-1])
    leftward = 0.5 * (center + padded[1:-1, :-2])
    rightward = 0.5 * (center + padded[1:-1, 2:])
    diagonal = 1.0 + upward + downward + leftward + rightward
    return upward, downward, leftward, rightward, diagonal


def relax_once(padded, source, terms):
    upward, downward, leftward, rightward, diagonal = terms
    total = source + upward * padded[:, :-2, 1:-1]
    total = total + downward * padded[:, 2:, 1:-1]
    total = total + leftward * padded[:, 1:-1, :-2]
    total = total + rightward * padded[:, 1:-1, 2:]
    return total / diagonal


def hdot(left, right):
    return jnp.dot(left, right, precision=lax.Precision.HIGHEST)


def reference(rhs_fields, coupling, inv_pivot, lower_factor, upper_factor):
    terms = face_terms(jnp.pad(coupling, 1))
    fine = rhs_fields
    for repeat in range(SWEEPS):
        fine = relax_once(jnp.pad(fine, ((0, 0), (1, 1), (1, 1))), rhs_fields, terms)
    sub_x = CX // SUB
    sub_y = CY // SUB
    coarse = rhs_fields.reshape(NRHS, N_ROW, SUB, sub_x, N_COL, SUB, sub_y).mean(axis=(3, 6))
    coarse = jnp.transpose(coarse, (1, 0, 3, 2, 4)).reshape(N_ROW, NRHS, NCB)

    def down_step(previous, inputs):
        block, pivot, lower = inputs
        value = hdot(block, pivot.T) - hdot(previous, lower.T)
        return value, value

    start = jnp.zeros((NRHS, NCB), jnp.float32)
    unused, downs = lax.scan(down_step, start, (coarse, inv_pivot, lower_factor))

    def back_step(following, inputs):
        value, upper = inputs
        solved = value - hdot(following, upper.T)
        return solved, solved

    unused, solved = lax.scan(back_step, start, (downs, upper_factor), reverse=True)
    solved = solved.reshape(N_ROW, NRHS, N_COL, SUB, SUB)
    solved = jnp.transpose(solved, (1, 0, 3, 2, 4))
    result = fine.reshape(NRHS, N_ROW, SUB, sub_x, N_COL, SUB, sub_y) + solved[:, :, :, None, :, :, None]
    return result.reshape(NRHS, NX, NY)
```

```python
import functools

import jax
import jax.numpy as jnp
from jax import lax
from jax.experimental import pallas as pl
from jax.experimental.pallas import tpu as pltpu
from jax.sharding import PartitionSpec as P

SWEEPS = 4
SUB = 8
LANES = 128
TILE = 8
VMEM = pl.BlockSpec(memory_space=pltpu.VMEM)
HIGHEST = lax.Precision.HIGHEST


def params():
    return pltpu.CompilerParams(vmem_limit_bytes=16 * 1024 * 1024)


def call(kernel, name, outs, scratch=(), flops=1_000_000):
    return pl.pallas_call(
        kernel,
        out_shape=outs,
        scratch_shapes=list(scratch),
        compiler_params=params(),
        cost_estimate=pl.CostEstimate(flops=flops, bytes_accessed=1_000_000, transcendentals=0),
        name=name,
    )


def f32(*shape):
    return jax.ShapeDtypeStruct(shape, jnp.float32)


def iota(shape, dim):
    return lax.broadcasted_iota(jnp.int32, shape, dim)


def thirds(value):
    first = value.astype(jnp.bfloat16)
    rest = value - first.astype(jnp.float32)
    second = rest.astype(jnp.bfloat16)
    third = (rest - second.astype(jnp.float32)).astype(jnp.bfloat16)
    return first, second, third


def selected(value, selector):
    return sum(
        jnp.dot(part, selector, preferred_element_type=jnp.float32) for part in thirds(value)
    )


def restrict_kernel(rhs_ref, coupling_ref, block_ref, low_ref, high_ref):
    count, extent_x, extent_y = rhs_ref.shape
    own = SUB * SUB
    pack = LANES // own
    sub_x, sub_y = extent_x // SUB, extent_y // SUB
    parts = []
    for b in range(count):
        cells = rhs_ref[b].reshape(SUB, sub_x // TILE, TILE, extent_y).sum(axis=1)
        parts.append(cells.reshape(SUB * TILE, extent_y))
    stacked = jnp.concatenate(parts, axis=0)
    shape = (extent_y, LANES)
    selector = (iota(shape, 0) // sub_y == iota(shape, 1) % SUB).astype(jnp.bfloat16)
    sums = selected(stacked, selector).reshape(count, SUB * TILE, LANES)
    lane = iota(sums.shape, 2)
    keep = (iota(sums.shape, 1) // TILE == (lane % own) // SUB) & (
        lane // own == lax.axis_index("col") % pack
    )
    block = jnp.where(keep, sums, 0.0).sum(axis=1) * (1.0 / (sub_x * sub_y))
    block_ref[...] = jnp.broadcast_to(block[None], block_ref.shape)
    for b in range(count + 1):
        field = rhs_ref.at[b] if b < count else coupling_ref
        low_ref[b] = field[:SWEEPS, :]
        high_ref[b] = field[extent_x - SWEEPS :, :]


def joined(gathered_ref, first, members, pack):
    blocks = []
    for p in range(members // pack):
        total = gathered_ref[first + pack * p]
        for q in range(1, pack):
            total = total + gathered_ref[first + pack * p + q]
        blocks.append(total)
    return jnp.concatenate(blocks, axis=1)


def product(gathered_ref, matrix_ref, offset):
    own, block = matrix_ref.shape[1:]
    members = block // own
    rows = gathered_ref.shape[0] // members
    first = 0
    if rows > 1:
        first = (lax.axis_index("row") + rows + offset) % rows * members
    values = joined(gathered_ref, first, members, LANES // own)
    return lax.dot_general(
        values,
        matrix_ref[0],
        (((1,), (1,)), ((), ())),
        precision=HIGHEST,
        preferred_element_type=jnp.float32,
    )


def place(own_values, block_ref):
    own = own_values.shape[1]
    pack = LANES // own
    wide = jnp.concatenate([own_values] * pack, axis=1)
    keep = iota(wide.shape, 1) // own == lax.axis_index("col") % pack
    block_ref[...] = jnp.broadcast_to(jnp.where(keep, wide, 0.0)[None], block_ref.shape)


def drive_kernel(gathered_ref, pivot_ref, own_ref, block_ref):
    values = product(gathered_ref, pivot_ref, 0)
    own_ref[...] = values
    place(values, block_ref)


def turn_kernel(turn, offset, gathered_ref, factor_ref, base_ref, stored_ref, own_ref, block_ref):
    update = base_ref[...] - product(gathered_ref, factor_ref, offset)
    values = jnp.where(lax.axis_index("row") == turn, update, stored_ref[...])
    own_ref[...] = values
    place(values, block_ref)


def finish_kernel(turn, gathered_ref, factor_ref, base_ref, stored_ref, fine_ref, out_ref):
    values = stored_ref[...]
    if turn is not None:
        update = base_ref[...] - product(gathered_ref, factor_ref, 1)
        values = jnp.where(lax.axis_index("row") == turn, update, values)
    count, extent_x, extent_y = fine_ref.shape
    own = values.shape[1]
    sub_x, sub_y = extent_x // SUB, extent_y // SUB
    spread = jnp.broadcast_to(values[:, None, :], (count, SUB, own))
    spread = jnp.where(iota(spread.shape, 2) // SUB == iota(spread.shape, 1), spread, 0.0)
    shape = (own, extent_y)
    selector = (iota(shape, 0) % SUB == iota(shape, 1) // sub_y).astype(jnp.bfloat16)
    coarse = selected(spread.reshape(count * SUB, own), selector)
    for b in range(count):
        for r in range(SUB):
            line = coarse[b * SUB + r : b * SUB + r + 1, :]
            rows = slice(r * sub_x, (r + 1) * sub_x)
            out_ref[b, rows, :] = fine_ref[b, rows, :] + line


def pack_kernel(rhs_ref, coupling_ref, above_ref, below_ref, first_ref, last_ref):
    count, extent_x, extent_y = rhs_ref.shape
    tiles = extent_x // TILE
    lane = iota((TILE, LANES), 1)
    for b in range(count + 1):
        field = rhs_ref.at[b] if b < count else coupling_ref
        halo = jnp.concatenate([below_ref[b], above_ref[b]], axis=0)
        for target, start, edge in (
            (first_ref, 0, 0),
            (last_ref, extent_y - LANES, LANES - SWEEPS),
        ):
            packed = jnp.zeros((TILE, LANES), jnp.float32)
            for i in range(tiles + 1):
                if i < tiles:
                    tile = field[i * TILE : (i + 1) * TILE, start : start + LANES]
                else:
                    tile = halo[:, start : start + LANES]
                shift = (SWEEPS * i - edge) % LANES
                moved = pltpu.roll(tile, shift, 1) if shift else tile
                packed = jnp.where(lane // SWEEPS == i, moved, packed)
            target[b] = packed


def shifted(ref, index, t):
    width = ref.shape[-1]
    here = ref[index, pl.ds(pl.multiple_of(t * TILE, TILE), TILE), :]
    before = ref[index, pl.ds(pl.multiple_of((t - 1) * TILE, TILE), TILE), :]
    after = ref[index, pl.ds(pl.multiple_of((t + 1) * TILE, TILE), TILE), :]
    sub = iota(here.shape, 0)
    up = jnp.where(sub == 0, pltpu.roll(before, 1, 0), pltpu.roll(here, 1, 0))
    down = jnp.where(
        sub == TILE - 1, pltpu.roll(after, TILE - 1, 0), pltpu.roll(here, TILE - 1, 0)
    )
    left = pltpu.roll(here, 1, 1)
    right = pltpu.roll(here, width - 1, 1)
    return here, up, down, left, right


def fine_kernel(
    rhs_ref, coupling_ref, above_ref, below_ref, left_ref, right_ref, out_ref,
    first_ref, second_ref, scaled_ref, face_ref,
):
    count, extent_x, extent_y = rhs_ref.shape
    tiles = extent_x // TILE
    width = extent_y + LANES
    lane = iota((TILE, LANES), 1)
    sub = iota((TILE, LANES), 0)
    blank = jnp.zeros((TILE, width), jnp.float32)
    for b in range(count + 1):
        field = rhs_ref.at[b] if b < count else coupling_ref
        for edge in (0, tiles + 3):
            first_ref[b, edge * TILE : (edge + 1) * TILE, :] = blank
            if b < count:
                second_ref[b, edge * TILE : (edge + 1) * TILE, :] = blank
        none = jnp.zeros((SWEEPS, extent_y), jnp.float32)
        first_ref[b, TILE : 2 * TILE, :extent_y] = jnp.concatenate([none, above_ref[b]], axis=0)
        first_ref[b, 2 * TILE : (2 + tiles) * TILE, :extent_y] = field[...]
        last = (2 + tiles) * TILE
        first_ref[b, last : last + TILE, :extent_y] = jnp.concatenate([below_ref[b], none], axis=0)
        for i in range(tiles + 1):
            low = pltpu.roll(right_ref[b], (-SWEEPS * i) % LANES, 1) if i else right_ref[b]
            high = pltpu.roll(left_ref[b], (LANES - SWEEPS - SWEEPS * i) % LANES, 1)
            tile = jnp.where(lane < SWEEPS, low, jnp.where(lane >= LANES - SWEEPS, high, 0.0))
            if i < tiles:
                place_at = (2 + i) * TILE
                first_ref[b, place_at : place_at + TILE, extent_y:] = tile
            else:
                half = TILE // 2
                first_ref[b, TILE : 2 * TILE, extent_y:] = jnp.where(sub >= half, tile, 0.0)
                first_ref[b, last : last + TILE, extent_y:] = jnp.where(sub < half, tile, 0.0)

    total_x = extent_x * lax.axis_size("row")
    total_y = extent_y * lax.axis_size("col")
    wide = (TILE, width)
    column = iota(wide, 1)
    own_y = jnp.where(column < extent_y + SWEEPS, column, column - width)
    global_y = own_y + lax.axis_index("col") * extent_y
    inside_y = (own_y >= -SWEEPS) & (global_y >= 0) & (global_y < total_y)

    def prepare(t, unused):
        here, up, down, left, right = shifted(first_ref, count, t)
        up = 0.5 * (here + up)
        down = 0.5 * (here + down)
        left = 0.5 * (here + left)
        right = 0.5 * (here + right)
        diagonal = 1.0 + up + down + left + right
        global_x = lax.axis_index("row") * extent_x + (t - 2) * TILE + iota(wide, 0)
        inside = inside_y & (global_x >= 0) & (global_x < total_x)
        inverse = jnp.where(inside, 1.0, 0.0) / diagonal
        rows = pl.ds(pl.multiple_of(t * TILE, TILE), TILE)
        for index, face in enumerate((up, down, left, right)):
            face_ref[index, rows, :] = face * inverse
        for b in range(count):
            scaled_ref[b, rows, :] = first_ref[b, rows, :] * inverse
        return unused

    lax.fori_loop(1, tiles + 3, prepare, 0)

    def relax(source, t, b):
        rows = pl.ds(pl.multiple_of(t * TILE, TILE), TILE)
        here, up, down, left, right = shifted(source, b, t)
        total = scaled_ref[b, rows, :] + face_ref[0, rows, :] * up
        total = total + face_ref[1, rows, :] * down
        total = total + face_ref[2, rows, :] * left
        return total + face_ref[3, rows, :] * right

    buffers = (first_ref, second_ref)
    for sweep in range(SWEEPS - 1):
        source, target = buffers[sweep % 2], buffers[(sweep + 1) % 2]

        def step(t, unused, source=source, target=target):
            rows = pl.ds(pl.multiple_of(t * TILE, TILE), TILE)
            for b in range(count):
                target[b, rows, :] = relax(source, t, b)
            return unused

        lax.fori_loop(1, tiles + 3, step, 0)

    def close(t, unused):
        rows = pl.ds(pl.multiple_of((t - 2) * TILE, TILE), TILE)
        for b in range(count):
            out_ref[b, rows, :] = relax(buffers[(SWEEPS - 1) % 2], t, b)[:, :extent_y]
        return unused

    lax.fori_loop(2, tiles + 2, close, 0)


def on_device(rhs_fields, coupling, inv_pivot, lower_factor, upper_factor):
    count, extent_x, extent_y = rhs_fields.shape
    own, block = inv_pivot.shape[1:]
    rows, columns = lax.axis_size("row"), lax.axis_size("col")
    row = lax.axis_index("row")
    both = ("row", "col")

    coarse, low, high = call(
        restrict_kernel,
        "restrict",
        (
            f32(columns, count, LANES),
            f32(count + 1, SWEEPS, extent_y),
            f32(count + 1, SWEEPS, extent_y),
        ),
    )(rhs_fields, coupling)
    gathered = lax.all_to_all(coarse, "col", 0, 0)

    if rows == 2:
        other = lax.ppermute(jnp.where(row == 0, high, low), "row", [(0, 1), (1, 0)])
        above = jnp.where(row == 0, 0.0, other)
        below = jnp.where(row == 0, other, 0.0)
    else:
        above = lax.ppermute(high, "row", [(i, i + 1) for i in range(rows - 1)])
        below = lax.ppermute(low, "row", [(i + 1, i) for i in range(rows - 1)])
    edge = f32(count + 1, TILE, LANES)
    first, last = call(pack_kernel, "pack", (edge, edge))(rhs_fields, coupling, above, below)
    left = lax.ppermute(last, "col", [(i, i + 1) for i in range(columns - 1)])
    right = lax.ppermute(first, "col", [(i + 1, i) for i in range(columns - 1)])
    tall = extent_x + 4 * TILE
    wide = extent_y + LANES
    fine = call(
        fine_kernel,
        "fine",
        f32(count, extent_x, extent_y),
        (
            pltpu.VMEM((count + 1, tall, wide), jnp.float32),
            pltpu.VMEM((count, tall, wide), jnp.float32),
            pltpu.VMEM((count, tall, wide), jnp.float32),
            pltpu.VMEM((4, tall, wide), jnp.float32),
        ),
        flops=20_000_000,
    )(rhs_fields, coupling, above, below, left, right)

    results = (f32(count, own), f32(rows * columns, count, LANES))
    driven, blocks = call(drive_kernel, "drive", results)(gathered, inv_pivot)
    stored = driven
    for turn in range(1, rows):
        gathered = lax.all_to_all(blocks, both, 0, 0)
        stored, blocks = call(
            functools.partial(turn_kernel, turn, -1), f"forward{turn}", results
        )(gathered, lower_factor, driven, stored)
    downs = stored
    for turn in range(rows - 2, 0, -1):
        gathered = lax.all_to_all(blocks, both, 0, 0)
        stored, blocks = call(
            functools.partial(turn_kernel, turn, 1), f"backward{turn}", results
        )(gathered, upper_factor, downs, stored)
    last_turn = None
    if rows > 1:
        gathered = lax.all_to_all(blocks, both, 0, 0)
        last_turn = 0
    return call(
        functools.partial(finish_kernel, last_turn), "finish", f32(count, extent_x, extent_y)
    )(gathered, upper_factor, downs, stored, fine)


def solution(mesh):
    return jax.shard_map(
        on_device,
        mesh=mesh,
        in_specs=(
            P(None, "row", "col"),
            P("row", "col"),
            P("row", "col", None),
            P("row", "col", None),
            P("row", "col", None),
        ),
        out_specs=P(None, "row", "col"),
        check_vma=False,
    )
```
